32 devices in a mesh: grp: 2 (over core), dev: 16 (over z, y, x).
Axes of the slice: x: 2, y: 2, z: 4, core: 2. Of those that a mesh axis runs over, the one named last changes fastest.
Arguments:
- coarse_emb: bfloat16 [16384, 128], P('dev'), may hold values from -6 to 6
- req_ids: int32 [16, 2, 16, 16], P('dev', 'grp'), may hold values from 0 to 1023, as said below
- fine_slot: int32 [16, 2, 2048], P('dev', 'grp'), may hold values from 0 to 255, as said below
- tiles: bfloat16 [512, 2, 8, 128, 128], P('dev', 'grp'), may hold values from -0.125 to 0.125
- tile_cols: int32 [512, 2, 8], P('dev', 'grp'), may hold values from 0 to 47
Outputs:
- smoothed: bfloat16 [65536, 128], P('dev')
The draws below stay inside these ranges and needn't reach their ends.
Inputs may be any that keep to these rules, and one draw needn't show every extreme that they name: For each d, g and o only the first entries of req_ids[d, g, o] are requested, at most 16 of them, and for each d and g some owner o has all 16; the remaining entries are 0. fine_slot[d, g, i] = o * 16 + j always names a requested entry j of req_ids[d, g, o], and every requested entry is named by some fine node.
All inputs are finite; a program needn't handle non-finite values.
Results may differ from the reference program's by a relative error of at most 0.001.
Values may be sent and summed in bfloat16 or wider, within the bound.
A program may use at most 64 MiB of HBM per device.

```python
import jax
import jax.numpy as jnp
from jax import lax

W = 128
B = 128
TPR = 8
CAP = 16
FINE_DEV = 4096
COARSE_DEV = 1024
HALF = 2048
NB = 32
F = 65536
NC = 16384
NBT = 512
N_GRP = 2
N_DEV = 16


def request_plan(key):
    base_key = jax.random.fold_in(key, 4242)
    k_count, k_heavy, k_start, k_stride = jax.random.split(base_key, 4)
    half_rows = FINE_DEV // N_GRP
    most_live = min(CAP, (half_rows - CAP) // max(N_DEV - 1, 1))
    least_live = min(CAP // 2, most_live)
    counts = jax.random.randint(k_count, (N_DEV, N_GRP, N_DEV), least_live, most_live + 1)
    heavy_owner = jax.random.randint(k_heavy, (N_DEV, N_GRP, 1), 0, N_DEV)
    owner_ids = jnp.arange(N_DEV, dtype=jnp.int32)
    counts = jnp.where(owner_ids[None, None, :] == heavy_owner, CAP, counts)
    start_row = jax.random.randint(k_start, (N_DEV, N_GRP, N_DEV, 1), 0, COARSE_DEV)
    stride = 2 * jax.random.randint(k_stride, (N_DEV, N_GRP, N_DEV, 1), 0, COARSE_DEV // 2) + 1
    slot_ids = jnp.arange(CAP, dtype=jnp.int32)
    row_ids = (start_row + slot_ids[None, None, None, :] * stride) % COARSE_DEV
    live_slots = slot_ids[None, None, None, :] < counts[..., None]
    row_ids = jnp.where(live_slots, row_ids, 0)
    return (row_ids.astype(jnp.int32), live_slots)


def draw_req_ids(key, part):
    return request_plan(key)[0]


def draw_fine_slot(key, part):
    row_ids, live_slots = request_plan(key)
    k_fill, k_order = jax.random.split(jax.random.fold_in(key, 77), 2)
    half_rows = FINE_DEV // N_GRP
    row_count = N_DEV * N_GRP
    live_flat = live_slots.reshape(row_count, N_DEV * CAP).astype(jnp.int32)
    slot_order = jnp.argsort(1 - live_flat, axis=1, stable=True).astype(jnp.int32)
    live_count = jnp.sum(live_flat, axis=1)
    positions = jnp.arange(half_rows, dtype=jnp.int32)[None, :]
    extra_pick = jax.random.randint(k_fill, (row_count, half_rows), 0, live_count[:, None])
    slot_index = jnp.where(positions < live_count[:, None], positions, extra_pick)
    chosen = jnp.take_along_axis(slot_order, slot_index, axis=1)
    shuffle_keys = jax.random.randint(k_order, (row_count, half_rows), 0, 2 ** 16) * half_rows + positions
    shuffle = jnp.argsort(shuffle_keys, axis=1, stable=True)
    chosen = jnp.take_along_axis(chosen, shuffle, axis=1)
    return chosen.reshape(N_DEV, N_GRP, half_rows).astype(jnp.int32)


def plant(entries, stream_key, least, top_value):
    spot = [jax.random.randint(jax.random.fold_in(stream_key, axis), (), 0, length) for axis, length in enumerate(entries.shape)]
    widest = entries.shape.index(max(entries.shape))
    next_to = spot[:widest] + [(spot[widest] + 1) % entries.shape[widest]] + spot[widest + 1:]
    return entries.at[tuple(spot)].set(least).at[tuple(next_to)].set(top_value)


def block_scale(key, dims, cuts, smallest, high):
    def one(axis_at, parts):
        draws = jax.random.uniform(jax.random.fold_in(jax.random.fold_in(key, 6), axis_at), (parts,), jnp.float32, smallest / len(cuts), high / len(cuts))
        return jnp.repeat(jnp.exp(draws), dims[axis_at] // parts).reshape((-1,) + (1,) * (len(dims) - axis_at - 1))

    factor_of = one(*cuts[0])
    for cut in cuts[1:]:
        factor_of = factor_of * one(*cut)
    return factor_of


def bell_draw(key, shape, scale, bound, cuts=(), held_as=jnp.bfloat16):
    entries = jax.random.normal(key, shape, jnp.float32) * scale
    if len(cuts) > 0:
        entries = block_scale(key, shape, cuts, -0.22, 0.18) * entries
    return jnp.clip(entries, min=-bound, max=bound).astype(held_as)


def setup_inputs(seed: int = 0) -> dict:
    seeds = jax.random.split(jax.random.key(seed), 6)
    return {
        "coarse_emb": bell_draw(seeds[0], (NC, W), 1.0, 6.0, ((0, 16),)),
        "req_ids": draw_req_ids(jax.random.fold_in(seeds[5], 71), 0),
        "fine_slot": draw_fine_slot(jax.random.fold_in(seeds[5], 71), 0),
        "tiles": bell_draw(seeds[3], (NBT, N_GRP, TPR, B, B), (B * TPR * N_GRP) ** -0.5, 0.125, ((0, 16), (1, 2))),
        "tile_cols": plant(jax.random.randint(seeds[4], (NBT, N_GRP, TPR), 0, 3 * (HALF // B)), jax.random.fold_in(seeds[4], 1), 0, (3 * (HALF // B)) - 1).astype(jnp.int32),
    }


def reference(coarse_emb, req_ids, fine_slot, tiles, tile_cols):
    owners = jnp.arange(N_DEV, dtype=jnp.int32)[None, None, :, None] * COARSE_DEV
    table_ids = (req_ids + owners).reshape(N_DEV, N_GRP, N_DEV * CAP)
    parent = jnp.take_along_axis(table_ids, fine_slot, axis=2)
    lifted = coarse_emb[parent]
    half_blocks = HALF // B
    blocks = lifted.reshape(N_DEV, N_GRP, half_blocks, B, W)
    zero_rows = jnp.zeros((1, N_GRP, half_blocks, B, W), jnp.bfloat16)
    padded = jnp.concatenate([zero_rows, blocks, zero_rows], axis=0)

    def one_dev(device):
        window = lax.dynamic_slice_in_dim(padded, device, 3, 0)
        extended = jnp.transpose(window, (1, 0, 2, 3, 4)).reshape(N_GRP, 3 * half_blocks, B, W)
        dev_tiles = lax.dynamic_slice_in_dim(tiles, device * NB, NB, 0)
        dev_cols = lax.dynamic_slice_in_dim(tile_cols, device * NB, NB, 0)
        summed = jnp.zeros((NB, B, W), jnp.float32)
        for group in range(N_GRP):
            picked = extended[group][dev_cols[:, group]]
            summed = summed + jnp.einsum("rtij,rtjw->riw", dev_tiles[:, group].astype(jnp.float32), picked.astype(jnp.float32))
        return summed

    tile_sums = lax.map(one_dev, jnp.arange(N_DEV, dtype=jnp.int32)).reshape(F, W)
    result = lifted.reshape(F, W).astype(jnp.float32) - 0.5 * tile_sums
    return result.astype(jnp.bfloat16)
```

```python
import functools

import jax
import jax.numpy as jnp
from jax import lax
from jax.experimental import pallas as pl
from jax.experimental.pallas import tpu as pltpu
from jax.sharding import PartitionSpec as P

MESH = pl.DeviceIdType.MESH
STEP = 4


def kernel(
    n, cap, req_hbm, fs_hbm, coarse_hbm, cols_hbm, tiles_hbm, out_hbm,
    req_v, req_out, req_in, fs, coarse, cols, tiles, rows_pad, tab, onehot, ext,
    part_out, part_in, done,
    local_sem, req_send, req_recv, fs_send, fs_recv, row_send, row_recv,
    part_send, part_recv, fin_send, fin_recv, out_sem,
):
    me = lax.axis_index("dev")
    grp = lax.axis_index("grp")
    other = 1 - grp
    half_blocks = fs.shape[1]
    b = fs.shape[2]
    w = coarse.shape[1]
    slots = n * cap
    steps = half_blocks // STEP

    req_copy = pltpu.make_async_copy(req_hbm, req_v, local_sem.at[0])
    fs_copy = pltpu.make_async_copy(fs_hbm, fs.at[1], local_sem.at[1])
    coarse_copy = pltpu.make_async_copy(coarse_hbm, coarse, local_sem.at[2])
    cols_copy = pltpu.make_async_copy(cols_hbm, cols, local_sem.at[3])
    tiles_copy = pltpu.make_async_copy(tiles_hbm, tiles, local_sem.at[4])
    req_copy.start()
    fs_copy.start()
    coarse_copy.start()
    cols_copy.start()
    tiles_copy.start()

    barrier = pltpu.get_barrier_semaphore()
    pl.semaphore_signal(barrier, inc=1, device_id={"grp": other}, device_id_type=MESH)

    def greet(k, c):
        peer = lax.rem(me + k, n)
        pl.semaphore_signal(barrier, inc=1, device_id={"dev": peer}, device_id_type=MESH)
        return c

    lax.fori_loop(1, n, greet, 0)

    rows_pad[0] = jnp.zeros((cap, w), jnp.bfloat16)
    rows_pad[n + 1] = jnp.zeros((cap, w), jnp.bfloat16)

    @pl.when(me == 0)
    def _():
        fs[0] = jnp.zeros((half_blocks, b), jnp.int32)

    @pl.when(me == n - 1)
    def _():
        fs[2] = jnp.zeros((half_blocks, b), jnp.int32)

    req_copy.wait()

    def spread(o, c):
        req_out[o, :, 0:cap] = req_v[pl.ds(o, 1), :]
        return c

    lax.fori_loop(0, n, spread, 0)
    req_in[me, :, 0:cap] = req_v[pl.ds(me, 1), :]

    def build_onehot(side):
        def one(i, c):
            row = fs[side, pl.ds(i, 1), :].astype(jnp.float32)
            col = jnp.transpose(jnp.broadcast_to(row, (b, b)))
            lanes = lax.broadcasted_iota(jnp.int32, (b, b), 1).astype(jnp.float32)
            base = pl.multiple_of((side * half_blocks + i) * b, b)
            for q in range(slots // b):
                hit = jnp.where(col == lanes + float(q * b), 1.0, 0.0)
                onehot[pl.ds(base, b), q * b:(q + 1) * b] = hit.astype(jnp.bfloat16)
            return c

        lax.fori_loop(0, half_blocks, one, 0)

    fs_copy.wait()
    build_onehot(1)
    pl.semaphore_wait(barrier, n)

    def req_remote(k):
        peer = lax.rem(me + k, n)
        return pltpu.make_async_remote_copy(
            src_ref=req_out.at[peer], dst_ref=req_in.at[me],
            send_sem=req_send.at[k], recv_sem=req_recv.at[me],
            device_id={"dev": peer}, device_id_type=MESH,
        )

    def req_arrival(k):
        peer = lax.rem(me + k, n)
        return pltpu.make_async_remote_copy(
            src_ref=req_out.at[peer], dst_ref=req_in.at[peer],
            send_sem=req_send.at[k], recv_sem=req_recv.at[peer],
            device_id={"dev": peer}, device_id_type=MESH,
        )

    def send_req(k, c):
        req_remote(k).start()
        return c

    lax.fori_loop(1, n, send_req, 0)

    up = pltpu.make_async_remote_copy(
        src_ref=fs.at[1], dst_ref=fs.at[0], send_sem=fs_send.at[0], recv_sem=fs_recv.at[0],
        device_id={"dev": lax.rem(me + 1, n)}, device_id_type=MESH,
    )
    down = pltpu.make_async_remote_copy(
        src_ref=fs.at[1], dst_ref=fs.at[2], send_sem=fs_send.at[1], recv_sem=fs_recv.at[1],
        device_id={"dev": lax.rem(me + n - 1, n)}, device_id_type=MESH,
    )

    @pl.when(me < n - 1)
    def _():
        up.start()

    @pl.when(me > 0)
    def _():
        down.start()

    coarse_copy.wait()

    def wait_req(k, c):
        req_arrival(k).wait_recv()
        return c

    lax.fori_loop(1, n, wait_req, 0)

    owned = coarse.shape[0]
    group = min(16, n)

    def gather(i, c):
        ids = req_in[pl.ds(i * group, group)].astype(jnp.float32)
        ids = jnp.broadcast_to(ids, (group, cap, ids.shape[2]))
        slot = lax.broadcasted_iota(jnp.int32, ids.shape, 1)
        lane = lax.broadcasted_iota(jnp.int32, ids.shape, 2)
        col = jnp.sum(jnp.where(slot == lane, ids, 0.0), axis=2, keepdims=True)
        col = col.reshape(group * cap, 1)
        node = lax.broadcasted_iota(jnp.int32, (group * cap, owned), 1).astype(jnp.float32)
        hit = jnp.where(col == node, 1.0, 0.0).astype(jnp.bfloat16)
        rows = jnp.dot(hit, coarse[...], preferred_element_type=jnp.float32)
        rows_pad[pl.ds(1 + i * group, group)] = rows.astype(jnp.bfloat16).reshape(group, cap, w)
        return c

    lax.fori_loop(0, n // group, gather, 0)

    def row_remote(k):
        peer = lax.rem(me + k, n)
        return pltpu.make_async_remote_copy(
            src_ref=rows_pad.at[pl.ds(peer, 3)], dst_ref=tab.at[me],
            send_sem=row_send.at[k], recv_sem=row_recv.at[me],
            device_id={"dev": peer}, device_id_type=MESH,
        )

    def row_arrival(k):
        peer = lax.rem(me + k, n)
        return pltpu.make_async_remote_copy(
            src_ref=rows_pad.at[pl.ds(peer, 3)], dst_ref=tab.at[peer],
            send_sem=row_send.at[k], recv_sem=row_recv.at[peer],
            device_id={"dev": peer}, device_id_type=MESH,
        )

    def send_rows(k, c):
        row_remote(k).start()
        return c

    lax.fori_loop(1, n, send_rows, 0)
    tab[me] = rows_pad[pl.ds(me, 3)]

    @pl.when(me > 0)
    def _():
        up.wait_recv()

    build_onehot(0)

    @pl.when(me < n - 1)
    def _():
        down.wait_recv()

    build_onehot(2)

    def wait_rows(k, c):
        row_arrival(k).wait_recv()
        return c

    lax.fori_loop(1, n, wait_rows, 0)

    for side in range(3):
        table = tab[:, side].reshape(slots, w)

        def lift(i, c, side=side, table=table):
            first = side * half_blocks + i * STEP
            hits = onehot[pl.ds(pl.multiple_of(first * b, b), STEP * b), :]
            rows = jnp.dot(hits, table, preferred_element_type=jnp.float32)
            ext[pl.ds(first, STEP)] = rows.astype(jnp.bfloat16).reshape(STEP, b, w)
            return c

        lax.fori_loop(0, steps, lift, 0)

    cols_copy.wait()
    tiles_copy.wait()
    tpr = tiles.shape[1]

    def tile_sum(r):
        lhs = jnp.concatenate([tiles[r, t] for t in range(tpr)], axis=1)
        rhs = jnp.concatenate([ext[cols[t, r]] for t in range(tpr)], axis=0)
        return jnp.dot(lhs, rhs, preferred_element_type=jnp.float32)

    def part_copy(i):
        return pltpu.make_async_remote_copy(
            src_ref=part_out.at[pl.ds(i * STEP, STEP)], dst_ref=part_in.at[pl.ds(i * STEP, STEP)],
            send_sem=part_send.at[i], recv_sem=part_recv.at[i],
            device_id={"grp": other}, device_id_type=MESH,
        )

    def give(i, c):
        for j in range(STEP):
            r = i * STEP + j
            part_out[r] = tile_sum(other * half_blocks + r)
        part_copy(i).start()
        return c

    lax.fori_loop(0, steps, give, 0)

    def fin_copy(i):
        rows = pl.ds(grp * half_blocks + i * STEP, STEP)
        return pltpu.make_async_remote_copy(
            src_ref=done.at[rows], dst_ref=done.at[rows],
            send_sem=fin_send.at[i], recv_sem=fin_recv.at[i],
            device_id={"grp": other}, device_id_type=MESH,
        )

    def fin_arrival(i):
        rows = pl.ds(other * half_blocks + i * STEP, STEP)
        return pltpu.make_async_remote_copy(
            src_ref=done.at[rows], dst_ref=done.at[rows],
            send_sem=fin_send.at[i], recv_sem=fin_recv.at[i],
            device_id={"grp": other}, device_id_type=MESH,
        )

    def own_out(i):
        rows = pl.ds(grp * half_blocks + i * STEP, STEP)
        return pltpu.make_async_copy(done.at[rows], out_hbm.at[rows], out_sem.at[0, i])

    def other_out(i):
        rows = pl.ds(other * half_blocks + i * STEP, STEP)
        return pltpu.make_async_copy(done.at[rows], out_hbm.at[rows], out_sem.at[1, i])

    def finish(i, c):
        part_copy(i).wait_recv()
        for j in range(STEP):
            r = i * STEP + j
            total = tile_sum(grp * half_blocks + r) + part_in[r]
            value = ext[half_blocks + r].astype(jnp.float32) - 0.5 * total
            done[grp * half_blocks + r] = value.astype(jnp.bfloat16)
        fin_copy(i).start()
        own_out(i).start()
        return c

    lax.fori_loop(0, steps, finish, 0)

    def collect(i, c):
        fin_arrival(i).wait_recv()
        other_out(i).start()
        return c

    lax.fori_loop(0, steps, collect, 0)

    def drain_peer(k, c):
        req_remote(k).wait_send()
        row_remote(k).wait_send()
        return c

    lax.fori_loop(1, n, drain_peer, 0)

    @pl.when(me < n - 1)
    def _():
        up.wait_send()

    @pl.when(me > 0)
    def _():
        down.wait_send()

    def drain_step(i, c):
        part_copy(i).wait_send()
        fin_copy(i).wait_send()
        own_out(i).wait()
        other_out(i).wait()
        return c

    lax.fori_loop(0, steps, drain_step, 0)


def per_device(coarse_emb, req_ids, fine_slot, tiles, tile_cols):
    n = lax.axis_size("dev")
    cap = req_ids.shape[3]
    owned, w = coarse_emb.shape
    row_blocks, _, tpr, b, _ = tiles.shape
    half_rows = fine_slot.shape[2]
    half_blocks = half_rows // b
    steps = half_blocks // STEP
    slots = n * cap
    dma = pltpu.SemaphoreType.DMA
    out = pl.pallas_call(
        functools.partial(kernel, n, cap),
        out_shape=jax.ShapeDtypeStruct((row_blocks, b, w), jnp.bfloat16),
        in_specs=[pl.BlockSpec(memory_space=pl.ANY)] * 5,
        out_specs=pl.BlockSpec(memory_space=pl.ANY),
        scratch_shapes=[
            pltpu.VMEM((n, cap), jnp.int32),
            pltpu.VMEM((n, 1, 128), jnp.int32),
            pltpu.VMEM((n, 1, 128), jnp.int32),
            pltpu.VMEM((3, half_blocks, b), jnp.int32),
            pltpu.VMEM((owned, w), jnp.bfloat16),
            pltpu.SMEM((tpr, row_blocks), jnp.int32),
            pltpu.VMEM((row_blocks, tpr, b, b), jnp.bfloat16),
            pltpu.VMEM((n + 2, cap, w), jnp.bfloat16),
            pltpu.VMEM((n, 3, cap, w), jnp.bfloat16),
            pltpu.VMEM((3 * half_rows, slots), jnp.bfloat16),
            pltpu.VMEM((3 * half_blocks, b, w), jnp.bfloat16),
            pltpu.VMEM((half_blocks, b, w), jnp.float32),
            pltpu.VMEM((half_blocks, b, w), jnp.float32),
            pltpu.VMEM((row_blocks, b, w), jnp.bfloat16),
            dma((5,)),
            dma((n,)),
            dma((n,)),
            dma((2,)),
            dma((2,)),
            dma((n,)),
            dma((n,)),
            dma((steps,)),
            dma((steps,)),
            dma((steps,)),
            dma((steps,)),
            dma((2, steps)),
        ],
        compiler_params=pltpu.CompilerParams(
            collective_id=0, has_side_effects=True, vmem_limit_bytes=60 * 1024 * 1024
        ),
    )(
        req_ids[0, 0],
        fine_slot.reshape(half_blocks, b),
        coarse_emb,
        tile_cols[:, 0].T,
        tiles[:, 0],
    )
    return out.reshape(row_blocks * b, w)


def solution(mesh):
    return jax.shard_map(
        per_device,
        mesh=mesh,
        in_specs=(
            P("dev", None),
            P("dev", "grp", None, None),
            P("dev", "grp", None),
            P("dev", "grp", None, None, None),
            P("dev", "grp", None),
        ),
        out_specs=P("dev", None),
        check_vma=False,
    )
```

```python
import functools

import jax
import jax.numpy as jnp
from jax import lax
from jax.experimental import pallas as pl
from jax.experimental.pallas import tpu as pltpu
from jax.sharding import PartitionSpec as P

MESH = pl.DeviceIdType.MESH
LIFT = 16
GIVE = 4
KEEP = 4


def kernel(
    n, cap, req_hbm, fs_hbm, coarse_hbm, cols_hbm, tiles_hbm, done,
    req_v, req_out, req_in, fs, coarse, cols, tiles, rows_pad, tab, onehot, ext,
    part_out, part_in,
    local_sem, req_send, req_recv, fs_send, fs_recv, row_send, row_recv,
    part_send, part_recv, fin_send, fin_recv,
):
    me = lax.axis_index("dev")
    grp = lax.axis_index("grp")
    other = 1 - grp
    half_blocks = fs.shape[1]
    b = fs.shape[2]
    w = coarse.shape[1]
    slots = n * cap
    req_copy = pltpu.make_async_copy(req_hbm, req_v, local_sem.at[0])
    fs_copy = pltpu.make_async_copy(fs_hbm, fs.at[1], local_sem.at[1])
    coarse_copy = pltpu.make_async_copy(coarse_hbm, coarse, local_sem.at[2])
    cols_copy = pltpu.make_async_copy(cols_hbm, cols, local_sem.at[3])
    tiles_copy = pltpu.make_async_copy(tiles_hbm, tiles, local_sem.at[4])
    req_copy.start()
    fs_copy.start()
    coarse_copy.start()
    cols_copy.start()
    tiles_copy.start()

    barrier = pltpu.get_barrier_semaphore()
    pl.semaphore_signal(barrier, inc=1, device_id={"grp": other}, device_id_type=MESH)

    def greet(k, c):
        peer = lax.rem(me + k, n)
        pl.semaphore_signal(barrier, inc=1, device_id={"dev": peer}, device_id_type=MESH)
        return c

    lax.fori_loop(1, n, greet, 0)

    rows_pad[0] = jnp.zeros((cap, w), jnp.bfloat16)
    rows_pad[n + 1] = jnp.zeros((cap, w), jnp.bfloat16)

    @pl.when(me == 0)
    def _():
        fs[0] = jnp.zeros((half_blocks, b), jnp.int32)

    @pl.when(me == n - 1)
    def _():
        fs[2] = jnp.zeros((half_blocks, b), jnp.int32)

    req_copy.wait()

    def spread(o, c):
        req_out[o, :, 0:cap] = req_v[pl.ds(o, 1), :]
        return c

    lax.fori_loop(0, n, spread, 0)
    req_in[me, :, 0:cap] = req_v[pl.ds(me, 1), :]

    def build_onehot(side):
        def one(i, c):
            row = fs[side, pl.ds(i, 1), :].astype(jnp.float32)
            col = jnp.transpose(jnp.broadcast_to(row, (b, b)))
            lanes = lax.broadcasted_iota(jnp.int32, (b, b), 1).astype(jnp.float32)
            base = pl.multiple_of((side * half_blocks + i) * b, b)
            for q in range(slots // b):
                hit = jnp.where(col == lanes + float(q * b), 1.0, 0.0)
                onehot[pl.ds(base, b), q * b:(q + 1) * b] = hit.astype(jnp.bfloat16)
            return c

        lax.fori_loop(0, half_blocks, one, 0)

    fs_copy.wait()
    build_onehot(1)
    pl.semaphore_wait(barrier, n)

    def req_remote(k):
        peer = lax.rem(me + k, n)
        return pltpu.make_async_remote_copy(
            src_ref=req_out.at[peer], dst_ref=req_in.at[me],
            send_sem=req_send.at[k], recv_sem=req_recv.at[me],
            device_id={"dev": peer}, device_id_type=MESH,
        )

    def req_arrival(k):
        peer = lax.rem(me + k, n)
        return pltpu.make_async_remote_copy(
            src_ref=req_out.at[peer], dst_ref=req_in.at[peer],
            send_sem=req_send.at[k], recv_sem=req_recv.at[peer],
            device_id={"dev": peer}, device_id_type=MESH,
        )

    def send_req(k, c):
        req_remote(k).start()
        return c

    lax.fori_loop(1, n, send_req, 0)

    up = pltpu.make_async_remote_copy(
        src_ref=fs.at[1], dst_ref=fs.at[0], send_sem=fs_send.at[0], recv_sem=fs_recv.at[0],
        device_id={"dev": lax.rem(me + 1, n)}, device_id_type=MESH,
    )
    down = pltpu.make_async_remote_copy(
        src_ref=fs.at[1], dst_ref=fs.at[2], send_sem=fs_send.at[1], recv_sem=fs_recv.at[1],
        device_id={"dev": lax.rem(me + n - 1, n)}, device_id_type=MESH,
    )

    @pl.when(me < n - 1)
    def _():
        up.start()

    @pl.when(me > 0)
    def _():
        down.start()

    coarse_copy.wait()

    def wait_req(k, c):
        req_arrival(k).wait_recv()
        return c

    lax.fori_loop(1, n, wait_req, 0)

    owned = coarse.shape[0]
    group = min(16, n)

    def gather(i, c):
        ids = req_in[pl.ds(i * group, group)].astype(jnp.float32)
        ids = jnp.broadcast_to(ids, (group, cap, ids.shape[2]))
        slot = lax.broadcasted_iota(jnp.int32, ids.shape, 1)
        lane = lax.broadcasted_iota(jnp.int32, ids.shape, 2)
        col = jnp.sum(jnp.where(slot == lane, ids, 0.0), axis=2, keepdims=True)
        col = col.reshape(group * cap, 1)
        node = lax.broadcasted_iota(jnp.int32, (group * cap, owned), 1).astype(jnp.float32)
        hit = jnp.where(col == node, 1.0, 0.0).astype(jnp.bfloat16)
        rows = jnp.dot(hit, coarse[...], preferred_element_type=jnp.float32)
        rows_pad[pl.ds(1 + i * group, group)] = rows.astype(jnp.bfloat16).reshape(group, cap, w)
        return c

    lax.fori_loop(0, n // group, gather, 0)

    def row_remote(k):
        peer = lax.rem(me + k, n)
        return pltpu.make_async_remote_copy(
            src_ref=rows_pad.at[pl.ds(peer, 3)], dst_ref=tab.at[me],
            send_sem=row_send.at[k], recv_sem=row_recv.at[me],
            device_id={"dev": peer}, device_id_type=MESH,
        )

    def row_arrival(k):
        peer = lax.rem(me + k, n)
        return pltpu.make_async_remote_copy(
            src_ref=rows_pad.at[pl.ds(peer, 3)], dst_ref=tab.at[peer],
            send_sem=row_send.at[k], recv_sem=row_recv.at[peer],
            device_id={"dev": peer}, device_id_type=MESH,
        )

    def send_rows(k, c):
        row_remote(k).start()
        return c

    lax.fori_loop(1, n, send_rows, 0)
    tab[me] = rows_pad[pl.ds(me, 3)]

    @pl.when(me > 0)
    def _():
        up.wait_recv()

    build_onehot(0)

    @pl.when(me < n - 1)
    def _():
        down.wait_recv()

    build_onehot(2)

    def wait_rows(k, c):
        row_arrival(k).wait_recv()
        return c

    lax.fori_loop(1, n, wait_rows, 0)

    for side in range(3):
        table = tab[:, side].reshape(slots, w)

        def lift(i, c, side=side, table=table):
            first = side * half_blocks + i * LIFT
            hits = onehot[pl.ds(pl.multiple_of(first * b, b), LIFT * b), :]
            rows = jnp.dot(hits, table, preferred_element_type=jnp.float32)
            ext[pl.ds(first, LIFT)] = rows.astype(jnp.bfloat16).reshape(LIFT, b, w)
            return c

        lax.fori_loop(0, half_blocks // LIFT, lift, 0)

    cols_copy.wait()
    tiles_copy.wait()
    tpr = tiles.shape[1]

    def tile_sum(r):
        lhs = jnp.concatenate([tiles[r, t] for t in range(tpr)], axis=1)
        rhs = jnp.concatenate([ext[cols[t, r]] for t in range(tpr)], axis=0)
        return jnp.dot(lhs, rhs, preferred_element_type=jnp.float32)

    def part_copy(i):
        return pltpu.make_async_remote_copy(
            src_ref=part_out.at[pl.ds(i * GIVE, GIVE)], dst_ref=part_in.at[pl.ds(i * GIVE, GIVE)],
            send_sem=part_send.at[i], recv_sem=part_recv.at[i],
            device_id={"grp": other}, device_id_type=MESH,
        )

    def give(i, c):
        for j in range(GIVE):
            r = i * GIVE + j
            part_out[r] = tile_sum(other * half_blocks + r)
        part_copy(i).start()
        return c

    lax.fori_loop(0, half_blocks // GIVE, give, 0)

    def fin_copy(i):
        rows = pl.ds(grp * half_blocks + i * KEEP, KEEP)
        return pltpu.make_async_remote_copy(
            src_ref=done.at[rows], dst_ref=done.at[rows],
            send_sem=fin_send.at[i], recv_sem=fin_recv.at[i],
            device_id={"grp": other}, device_id_type=MESH,
        )

    def fin_arrival(i):
        rows = pl.ds(other * half_blocks + i * KEEP, KEEP)
        return pltpu.make_async_remote_copy(
            src_ref=done.at[rows], dst_ref=done.at[rows],
            send_sem=fin_send.at[i], recv_sem=fin_recv.at[i],
            device_id={"grp": other}, device_id_type=MESH,
        )

    def finish(i, c):
        if KEEP < GIVE:
            @pl.when(lax.rem(i, GIVE // KEEP) == 0)
            def _():
                part_copy(i // (GIVE // KEEP)).wait_recv()
        else:
            part_copy(i).wait_recv()
        for j in range(KEEP):
            r = i * KEEP + j
            total = tile_sum(grp * half_blocks + r) + part_in[r]
            value = ext[half_blocks + r].astype(jnp.float32) - 0.5 * total
            done[grp * half_blocks + r] = value.astype(jnp.bfloat16)
        fin_copy(i).start()
        return c

    lax.fori_loop(0, half_blocks // KEEP, finish, 0)

    def drain_peer(k, c):
        req_remote(k).wait_send()
        row_remote(k).wait_send()
        return c

    lax.fori_loop(1, n, drain_peer, 0)

    @pl.when(me < n - 1)
    def _():
        up.wait_send()

    @pl.when(me > 0)
    def _():
        down.wait_send()

    def drain_give(i, c):
        part_copy(i).wait_send()
        return c

    lax.fori_loop(0, half_blocks // GIVE, drain_give, 0)

    def drain_keep(i, c):
        fin_copy(i).wait_send()
        fin_arrival(i).wait_recv()
        return c

    lax.fori_loop(0, half_blocks // KEEP, drain_keep, 0)


def per_device(coarse_emb, req_ids, fine_slot, tiles, tile_cols):
    n = lax.axis_size("dev")
    cap = req_ids.shape[3]
    owned, w = coarse_emb.shape
    row_blocks, _, tpr, b, _ = tiles.shape
    half_rows = fine_slot.shape[2]
    half_blocks = half_rows // b
    gives, keeps = half_blocks // GIVE, half_blocks // KEEP
    slots = n * cap
    dma = pltpu.SemaphoreType.DMA
    out = pl.pallas_call(
        functools.partial(kernel, n, cap),
        out_shape=pltpu.VMEM((row_blocks, b, w), jnp.bfloat16),
        in_specs=[pl.BlockSpec(memory_space=pl.ANY)] * 5,
        out_specs=pl.BlockSpec(memory_space=pltpu.VMEM),
        scratch_shapes=[
            pltpu.VMEM((n, cap), jnp.int32),
            pltpu.VMEM((n, 1, 128), jnp.int32),
            pltpu.VMEM((n, 1, 128), jnp.int32),
            pltpu.VMEM((3, half_blocks, b), jnp.int32),
            pltpu.VMEM((owned, w), jnp.bfloat16),
            pltpu.SMEM((tpr, row_blocks), jnp.int32),
            pltpu.VMEM((row_blocks, tpr, b, b), jnp.bfloat16),
            pltpu.VMEM((n + 2, cap, w), jnp.bfloat16),
            pltpu.VMEM((n, 3, cap, w), jnp.bfloat16),
            pltpu.VMEM((3 * half_rows, slots), jnp.bfloat16),
            pltpu.VMEM((3 * half_blocks, b, w), jnp.bfloat16),
            pltpu.VMEM((half_blocks, b, w), jnp.float32),
            pltpu.VMEM((half_blocks, b, w), jnp.float32),
            dma((5,)),
            dma((n,)),
            dma((n,)),
            dma((2,)),
            dma((2,)),
            dma((n,)),
            dma((n,)),
            dma((gives,)),
            dma((gives,)),
            dma((keeps,)),
            dma((keeps,)),
        ],
        compiler_params=pltpu.CompilerParams(
            collective_id=0, has_side_effects=True, vmem_limit_bytes=48 * 1024 * 1024
        ),
    )(*(
        pltpu.with_memory_space_constraint(x, pltpu.HBM)
        for x in (
            req_ids[0, 0],
            fine_slot.reshape(half_blocks, b),
            coarse_emb,
            tile_cols[:, 0].T,
            tiles[:, 0],
        )
    ))
    return out.reshape(row_blocks * b, w)


def solution(mesh):
    return jax.shard_map(
        per_device,
        mesh=mesh,
        in_specs=(
            P("dev", None),
            P("dev", "grp", None, None),
            P("dev", "grp", None),
            P("dev", "grp", None, None, None),
            P("dev", "grp", None),
        ),
        out_specs=P("dev", None),
        check_vma=False,
    )
```

```python
import functools

import jax
import jax.numpy as jnp
from jax import lax
from jax.experimental import pallas as pl
from jax.experimental.pallas import tpu as pltpu
from jax.sharding import PartitionSpec as P

MESH = pl.DeviceIdType.MESH
LIFT = 16
GIVE = 4
KEEP = 4


def wrapped(index, n):
    return jnp.where(index >= n, index - n, index)


def each_peer(n, body):
    if n <= 16:
        for k in range(1, n):
            body(k, 0)
    else:
        lax.fori_loop(1, n, body, 0)


def kernel(
    n, cap, req_hbm, fs_hbm, coarse_hbm, cols_hbm, tiles_hbm, done,
    req_v, req_out, req_in, fs, coarse, cols, tiles, rows_pad, tab, onehot, ext,
    part_out, part_in,
    local_sem, req_send, req_recv, fs_send, fs_recv, row_send, row_recv,
    part_send, part_recv, fin_send, fin_recv,
):
    me = lax.axis_index("dev")
    grp = lax.axis_index("grp")
    other = 1 - grp
    half_blocks = fs.shape[1]
    b = fs.shape[2]
    w = coarse.shape[1]
    slots = n * cap
    req_copy = pltpu.make_async_copy(req_hbm, req_v, local_sem.at[0])
    fs_copy = pltpu.make_async_copy(fs_hbm, fs.at[1], local_sem.at[1])
    coarse_copy = pltpu.make_async_copy(coarse_hbm, coarse, local_sem.at[2])
    cols_copy = pltpu.make_async_copy(cols_hbm, cols, local_sem.at[3])
    tiles_copy = pltpu.make_async_copy(tiles_hbm, tiles, local_sem.at[4])
    req_copy.start()
    fs_copy.start()
    coarse_copy.start()
    cols_copy.start()
    tiles_copy.start()

    barrier = pltpu.get_barrier_semaphore()
    pl.semaphore_signal(barrier, inc=1, device_id={"grp": other}, device_id_type=MESH)

    def greet(k, c):
        peer = wrapped(me + k, n)
        pl.semaphore_signal(barrier, inc=1, device_id={"dev": peer}, device_id_type=MESH)
        return c

    each_peer(n, greet)

    rows_pad[0] = jnp.zeros((cap, w), jnp.bfloat16)
    rows_pad[n + 1] = jnp.zeros((cap, w), jnp.bfloat16)

    @pl.when(me == 0)
    def _():
        fs[0] = jnp.zeros((half_blocks, b), jnp.int32)

    @pl.when(me == n - 1)
    def _():
        fs[2] = jnp.zeros((half_blocks, b), jnp.int32)

    req_copy.wait()

    def spread(o, c):
        req_out[o, :, 0:cap] = req_v[pl.ds(o, 1), :]
        return c

    lax.fori_loop(0, n, spread, 0)
    req_in[me, :, 0:cap] = req_v[pl.ds(me, 1), :]

    def build_onehot(side):
        def one(i, c):
            row = fs[side, pl.ds(i, 1), :].astype(jnp.float32)
            col = jnp.transpose(jnp.broadcast_to(row, (b, b)))
            lanes = lax.broadcasted_iota(jnp.int32, (b, b), 1).astype(jnp.float32)
            base = pl.multiple_of((side * half_blocks + i) * b, b)
            for q in range(slots // b):
                hit = jnp.where(col == lanes + float(q * b), 1.0, 0.0)
                onehot[pl.ds(base, b), q * b:(q + 1) * b] = hit.astype(jnp.bfloat16)
            return c

        lax.fori_loop(0, half_blocks, one, 0)

    fs_copy.wait()
    build_onehot(1)
    pl.semaphore_wait(barrier, n)

    def req_remote(k):
        peer = wrapped(me + k, n)
        return pltpu.make_async_remote_copy(
            src_ref=req_out.at[peer], dst_ref=req_in.at[me],
            send_sem=req_send.at[k], recv_sem=req_recv.at[me],
            device_id={"dev": peer}, device_id_type=MESH,
        )

    def req_arrival(k):
        peer = wrapped(me + k, n)
        return pltpu.make_async_remote_copy(
            src_ref=req_out.at[peer], dst_ref=req_in.at[peer],
            send_sem=req_send.at[k], recv_sem=req_recv.at[peer],
            device_id={"dev": peer}, device_id_type=MESH,
        )

    def send_req(k, c):
        req_remote(k).start()
        return c

    each_peer(n, send_req)

    up = pltpu.make_async_remote_copy(
        src_ref=fs.at[1], dst_ref=fs.at[0], send_sem=fs_send.at[0], recv_sem=fs_recv.at[0],
        device_id={"dev": lax.rem(me + 1, n)}, device_id_type=MESH,
    )
    down = pltpu.make_async_remote_copy(
        src_ref=fs.at[1], dst_ref=fs.at[2], send_sem=fs_send.at[1], recv_sem=fs_recv.at[1],
        device_id={"dev": lax.rem(me + n - 1, n)}, device_id_type=MESH,
    )

    @pl.when(me < n - 1)
    def _():
        up.start()

    @pl.when(me > 0)
    def _():
        down.start()

    coarse_copy.wait()

    def wait_req(k, c):
        req_arrival(k).wait_recv()
        return c

    lax.fori_loop(1, n, wait_req, 0)

    owned = coarse.shape[0]
    group = min(16, n)

    def gather(i, c):
        ids = req_in[pl.ds(i * group, group)].astype(jnp.float32)
        ids = jnp.broadcast_to(ids, (group, cap, ids.shape[2]))
        slot = lax.broadcasted_iota(jnp.int32, ids.shape, 1)
        lane = lax.broadcasted_iota(jnp.int32, ids.shape, 2)
        col = jnp.sum(jnp.where(slot == lane, ids, 0.0), axis=2, keepdims=True)
        col = col.reshape(group * cap, 1)
        node = lax.broadcasted_iota(jnp.int32, (group * cap, owned), 1).astype(jnp.float32)
        hit = jnp.where(col == node, 1.0, 0.0).astype(jnp.bfloat16)
        rows = jnp.dot(hit, coarse[...], preferred_element_type=jnp.float32)
        rows_pad[pl.ds(1 + i * group, group)] = rows.astype(jnp.bfloat16).reshape(group, cap, w)
        return c

    lax.fori_loop(0, n // group, gather, 0)

    def row_remote(k):
        peer = wrapped(me + k, n)
        return pltpu.make_async_remote_copy(
            src_ref=rows_pad.at[pl.ds(peer, 3)], dst_ref=tab.at[me],
            send_sem=row_send.at[k], recv_sem=row_recv.at[me],
            device_id={"dev": peer}, device_id_type=MESH,
        )

    def row_arrival(k):
        peer = wrapped(me + k, n)
        return pltpu.make_async_remote_copy(
            src_ref=rows_pad.at[pl.ds(peer, 3)], dst_ref=tab.at[peer],
            send_sem=row_send.at[k], recv_sem=row_recv.at[peer],
            device_id={"dev": peer}, device_id_type=MESH,
        )

    def send_rows(k, c):
        row_remote(k).start()
        return c

    each_peer(n, send_rows)
    tab[me] = rows_pad[pl.ds(me, 3)]

    @pl.when(me > 0)
    def _():
        up.wait_recv()

    build_onehot(0)

    @pl.when(me < n - 1)
    def _():
        down.wait_recv()

    build_onehot(2)

    def wait_rows(k, c):
        row_arrival(k).wait_recv()
        return c

    lax.fori_loop(1, n, wait_rows, 0)

    for side in range(3):
        table = tab[:, side].reshape(slots, w)

        def lift(i, c, side=side, table=table):
            first = side * half_blocks + i * LIFT
            hits = onehot[pl.ds(pl.multiple_of(first * b, b), LIFT * b), :]
            rows = jnp.dot(hits, table, preferred_element_type=jnp.float32)
            ext[pl.ds(first, LIFT)] = rows.astype(jnp.bfloat16).reshape(LIFT, b, w)
            return c

        lax.fori_loop(0, half_blocks // LIFT, lift, 0)

    cols_copy.wait()
    tiles_copy.wait()
    tpr = tiles.shape[1]

    def tile_sum(r):
        lhs = jnp.concatenate([tiles[r, t] for t in range(tpr)], axis=1)
        rhs = jnp.concatenate([ext[cols[t, r]] for t in range(tpr)], axis=0)
        return jnp.dot(lhs, rhs, preferred_element_type=jnp.float32)

    def part_copy(i):
        return pltpu.make_async_remote_copy(
            src_ref=part_out.at[pl.ds(i * GIVE, GIVE)], dst_ref=part_in.at[pl.ds(i * GIVE, GIVE)],
            send_sem=part_send.at[i], recv_sem=part_recv.at[i],
            device_id={"grp": other}, device_id_type=MESH,
        )

    def give(i, c):
        for j in range(GIVE):
            r = i * GIVE + j
            part_out[r] = tile_sum(other * half_blocks + r)
        part_copy(i).start()
        return c

    lax.fori_loop(0, half_blocks // GIVE, give, 0)

    def fin_copy(i):
        rows = pl.ds(grp * half_blocks + i * KEEP, KEEP)
        return pltpu.make_async_remote_copy(
            src_ref=done.at[rows], dst_ref=done.at[rows],
            send_sem=fin_send.at[i], recv_sem=fin_recv.at[i],
            device_id={"grp": other}, device_id_type=MESH,
        )

    def fin_arrival(i):
        rows = pl.ds(other * half_blocks + i * KEEP, KEEP)
        return pltpu.make_async_remote_copy(
            src_ref=done.at[rows], dst_ref=done.at[rows],
            send_sem=fin_send.at[i], recv_sem=fin_recv.at[i],
            device_id={"grp": other}, device_id_type=MESH,
        )

    def finish(i, c):
        if KEEP < GIVE:
            @pl.when(lax.rem(i, GIVE // KEEP) == 0)
            def _():
                part_copy(i // (GIVE // KEEP)).wait_recv()
        else:
            part_copy(i).wait_recv()
        for j in range(KEEP):
            r = i * KEEP + j
            total = tile_sum(grp * half_blocks + r) + part_in[r]
            value = ext[half_blocks + r].astype(jnp.float32) - 0.5 * total
            done[grp * half_blocks + r] = value.astype(jnp.bfloat16)
        fin_copy(i).start()
        return c

    lax.fori_loop(0, half_blocks // KEEP, finish, 0)

    def drain_peer(k, c):
        req_remote(k).wait_send()
        row_remote(k).wait_send()
        return c

    lax.fori_loop(1, n, drain_peer, 0)

    @pl.when(me < n - 1)
    def _():
        up.wait_send()

    @pl.when(me > 0)
    def _():
        down.wait_send()

    def drain_give(i, c):
        part_copy(i).wait_send()
        return c

    lax.fori_loop(0, half_blocks // GIVE, drain_give, 0)

    def drain_keep(i, c):
        fin_copy(i).wait_send()
        fin_arrival(i).wait_recv()
        return c

    lax.fori_loop(0, half_blocks // KEEP, drain_keep, 0)


def per_device(coarse_emb, req_ids, fine_slot, tiles, tile_cols):
    n = lax.axis_size("dev")
    cap = req_ids.shape[3]
    owned, w = coarse_emb.shape
    row_blocks, _, tpr, b, _ = tiles.shape
    half_rows = fine_slot.shape[2]
    half_blocks = half_rows // b
    gives, keeps = half_blocks // GIVE, half_blocks // KEEP
    slots = n * cap
    dma = pltpu.SemaphoreType.DMA
    out = pl.pallas_call(
        functools.partial(kernel, n, cap),
        out_shape=pltpu.VMEM((row_blocks, b, w), jnp.bfloat16),
        in_specs=[pl.BlockSpec(memory_space=pl.ANY)] * 5,
        out_specs=pl.BlockSpec(memory_space=pltpu.VMEM),
        scratch_shapes=[
            pltpu.VMEM((n, cap), jnp.int32),
            pltpu.VMEM((n, 1, 128), jnp.int32),
            pltpu.VMEM((n, 1, 128), jnp.int32),
            pltpu.VMEM((3, half_blocks, b), jnp.int32),
            pltpu.VMEM((owned, w), jnp.bfloat16),
            pltpu.SMEM((tpr, row_blocks), jnp.int32),
            pltpu.VMEM((row_blocks, tpr, b, b), jnp.bfloat16),
            pltpu.VMEM((n + 2, cap, w), jnp.bfloat16),
            pltpu.VMEM((n, 3, cap, w), jnp.bfloat16),
            pltpu.VMEM((3 * half_rows, slots), jnp.bfloat16),
            pltpu.VMEM((3 * half_blocks, b, w), jnp.bfloat16),
            pltpu.VMEM((half_blocks, b, w), jnp.float32),
            pltpu.VMEM((half_blocks, b, w), jnp.float32),
            dma((5,)),
            dma((n,)),
            dma((n,)),
            dma((2,)),
            dma((2,)),
            dma((n,)),
            dma((n,)),
            dma((gives,)),
            dma((gives,)),
            dma((keeps,)),
            dma((keeps,)),
        ],
        compiler_params=pltpu.CompilerParams(
            collective_id=0, has_side_effects=True, vmem_limit_bytes=48 * 1024 * 1024
        ),
    )(*(
        pltpu.with_memory_space_constraint(x, pltpu.HBM)
        for x in (
            req_ids[0, 0],
            fine_slot.reshape(half_blocks, b),
            coarse_emb,
            tile_cols[:, 0].T,
            tiles[:, 0],
        )
    ))
    return out.reshape(row_blocks * b, w)


def solution(mesh):
    return jax.shard_map(
        per_device,
        mesh=mesh,
        in_specs=(
            P("dev", None),
            P("dev", "grp", None, None),
            P("dev", "grp", None),
            P("dev", "grp", None, None, None),
            P("dev", "grp", None),
        ),
        out_specs=P("dev", None),
        check_vma=False,
    )
```
